32 devices in a mesh: section: 2 (over x), sht: 16 (over z, y, core).
Axes of the slice: x: 2, y: 2, z: 4, core: 2. Of those that a mesh axis runs over, the one named last changes fastest.
Arguments:
- analysis: bfloat16 [128, 256, 192], P('sht', None, 'section'), may hold values from -6 to 6
- perturbations: bfloat16 [6, 128, 256, 192], P(None, 'sht', None, 'section'), may hold values from -6 to 6
- gain_first: float32 [2, 192], P('section'), may hold values from 0.1 to 1.9
- spectral_gain: float32 [2, 2, 24576], P('section'), may hold values from -6 to 6
- skip_weight: bfloat16 [2, 192, 192], P('section'), may hold values from -0.4375 to 0.4375
- gain_second: float32 [2, 192], P('section'), may hold values from 0.1 to 1.9
- mlp_in: bfloat16 [2, 192, 384], P('section'), may hold values from -0.4375 to 0.4375
- mlp_out: bfloat16 [2, 192, 384], P('section'), may hold values from -0.3125 to 0.3125
Outputs:
- block_outputs: bfloat16 [2, 6, 128, 49152], P('section', None, 'sht')
The draws below stay inside these ranges and needn't reach their ends.
All inputs are finite; a program needn't handle non-finite values.
Results may differ from the reference program's by a relative error of at most 0.025.
Values may be sent and summed in bfloat16 or wider, within the bound.
A program may use at most 64 MiB of HBM per device.

```python
import math
import jax
import jax.numpy as jnp
from jax import lax

C = 192
HID = 384
NLAT = 128
NLON = 256
LMAX = 128
MMAX = 128
MEMBERS = 6
BLOCKS = 2
N_SECTION = 2


def level_of(stream_key, dims, shards, low, largest):
    def one(position, blocks):
        draws = jax.random.uniform(jax.random.fold_in(jax.random.fold_in(stream_key, 6), position), (blocks,), jnp.float32, low / len(shards), largest / len(shards))
        return jnp.repeat(jnp.exp(draws), dims[position] // blocks).reshape((-1,) + (1,) * (len(dims) - position - 1))

    gain = one(*shards[0])
    for cut in shards[1:]:
        gain = gain * one(*cut)
    return gain


def noise(own_key, shape, spread, most, cuts=(), held_as=jnp.bfloat16):
    result = jax.random.normal(own_key, shape, jnp.float32) * spread
    if len(cuts) > 0:
        result = level_of(own_key, shape, cuts, -0.22, 0.18) * result
    return jnp.clip(result, min=-most, max=most).astype(held_as)


def setup_inputs(seed: int = 0) -> dict:
    keys = jax.random.split(jax.random.key(seed), 9)
    return {
        "analysis": noise(keys[0], (NLAT, NLON, C), 1.0, 6.0, ((0, 16), (2, 2))),
        "perturbations": noise(keys[1], (MEMBERS, NLAT, NLON, C), 1.0, 6.0, ((1, 16), (3, 2))),
        "gain_first": jnp.clip(1.0 + 0.18 * jax.random.normal(keys[2], (BLOCKS, C), jnp.float32), 0.1, 1.9),
        "spectral_gain": noise(keys[3], (BLOCKS, 2, LMAX * C), 1.0, 6.0, ((0, 2),), jnp.float32),
        "skip_weight": noise(keys[4], (BLOCKS, C, C), C ** -0.5, 0.4375, ((0, 2),)),
        "gain_second": jnp.clip(1.0 + 0.18 * jax.random.normal(keys[5], (BLOCKS, C), jnp.float32), 0.1, 1.9),
        "mlp_in": noise(keys[6], (BLOCKS, C, HID), C ** -0.5, 0.4375, ((0, 2),)),
        "mlp_out": noise(keys[7], (BLOCKS, C, HID), HID ** -0.5, 0.3125, ((0, 2),)),
    }


def legendre_table(nlat, lmax, mmax, nlon, m_first, m_count):
    latitudes = jnp.arange(nlat, dtype=jnp.float32)
    colatitude = math.pi * (latitudes + 0.5) / nlat
    cosine = jnp.cos(colatitude)
    sine = jnp.sin(colatitude)
    orders = jnp.arange(1, mmax, dtype=jnp.float32)
    factors = jnp.cumsum(0.5 * jnp.log((2.0 * orders + 1.0) / (2.0 * orders)))
    log_diag = jnp.concatenate([jnp.zeros((1,), jnp.float32), factors])
    m_index = m_first + jnp.arange(m_count, dtype=jnp.int32)
    picked = lax.optimization_barrier(jnp.sum(jnp.where(m_index[:, None] == jnp.arange(mmax, dtype=jnp.int32)[None, :], log_diag[None, :], 0.0), axis=1))
    m_float = m_index.astype(jnp.float32)
    diagonal = jnp.exp(picked[None, :] + m_float[None, :] * jnp.log(sine)[:, None]) * math.sqrt(0.25 / math.pi)
    cos_col = cosine[:, None]

    def advance(carry, degree):
        latest, earlier = carry
        degree_float = degree.astype(jnp.float32)
        lower = jnp.sqrt((4.0 * degree_float * degree_float - 1.0) / jnp.maximum(degree_float * degree_float - m_float * m_float, 1.0))
        shifted = degree_float - 1.0
        upper = jnp.sqrt(jnp.maximum(shifted * shifted - m_float * m_float, 0.0) / jnp.maximum(4.0 * shifted * shifted - 1.0, 1.0))
        recurred = lower[None, :] * (cos_col * latest - upper[None, :] * earlier)
        first_step = jnp.sqrt(2.0 * m_float + 3.0)[None, :] * cos_col * diagonal
        current = jnp.where(degree == m_index[None, :], diagonal, jnp.where(degree == m_index[None, :] + 1, first_step, jnp.where(degree > m_index[None, :] + 1, recurred, 0.0)))
        return ((current, latest), current)
    initial = jnp.zeros((nlat, m_count), jnp.float32)
    _, stacked = lax.scan(advance, (initial, initial), jnp.arange(lmax, dtype=jnp.int32), unroll=8)
    legendre = jnp.transpose(stacked, (1, 0, 2))
    weights = sine * (2.0 * math.pi / nlon) * (math.pi / nlat)
    return (legendre, weights)

def fourier_tables(nlon, mmax):
    samples = jnp.arange(nlon, dtype=jnp.int32)
    orders = jnp.arange(mmax, dtype=jnp.int32)
    phase = (samples[:, None] * orders[None, :] % nlon).astype(jnp.float32) * (2.0 * math.pi / nlon)
    cosines = jnp.cos(phase)
    sines = jnp.sin(phase)
    forward = jnp.stack([cosines, -sines], axis=1).astype(jnp.bfloat16)
    factor = jnp.where(orders == 0, 1.0, 2.0).astype(jnp.float32)
    inverse = jnp.stack([cosines.T * factor[:, None], -sines.T * factor[:, None]], axis=0).astype(jnp.bfloat16)
    return (forward, inverse)

def layer_norm(values, gain_vector):
    average = lax.optimization_barrier(jnp.mean(values, axis=-1, keepdims=True))
    centred = values - average
    variance = lax.optimization_barrier(jnp.mean(centred * centred, axis=-1, keepdims=True))
    return centred * lax.rsqrt(variance + 1e-05) * gain_vector

def apply_gain(coeffs, gain_table):
    real_part = coeffs[:, :, :, 0]
    imag_part = coeffs[:, :, :, 1]
    gain_real = gain_table[0][None, :, None, :]
    gain_imag = gain_table[1][None, :, None, :]
    return jnp.stack([real_part * gain_real - imag_part * gain_imag, real_part * gain_imag + imag_part * gain_real], axis=3)

def project_out(hidden, out_matrix):
    return lax.dot_general(hidden, out_matrix, (((1,), (1,)), ((), ())), preferred_element_type=jnp.float32)

def sfno_block(current_state, gain_one, gain_flat, skip_matrix, gain_two, first_matrix, second_matrix, weighted, plain_table, forward, inverse):
    state_wide = current_state.astype(jnp.float32)
    channels = current_state.shape[-1]
    gain_table = gain_flat.reshape(2, -1, channels)
    normed = layer_norm(state_wide, gain_one).astype(jnp.bfloat16)
    spectrum = jnp.einsum('bjkc,kpm->bjmpc', normed.astype(jnp.float32), forward.astype(jnp.float32)).astype(jnp.bfloat16)
    coeffs = jnp.einsum('jlm,bjmpc->blmpc', weighted.astype(jnp.float32), spectrum.astype(jnp.float32))
    filtered = apply_gain(coeffs, gain_table).astype(jnp.bfloat16)
    returned = jnp.einsum('jlm,blmpc->bjmpc', plain_table.astype(jnp.float32), filtered.astype(jnp.float32)).astype(jnp.bfloat16)
    spatial = jnp.einsum('bjmpc,pmk->bjkc', returned.astype(jnp.float32), inverse.astype(jnp.float32))
    skipped = jnp.dot(normed.reshape(-1, channels), skip_matrix, preferred_element_type=jnp.float32).reshape(spatial.shape)
    activated = jax.nn.gelu(spatial + skipped, approximate=False)
    second = layer_norm(activated, gain_two).astype(jnp.bfloat16)
    hidden = jax.nn.gelu(jnp.dot(second.reshape(-1, channels), first_matrix, preferred_element_type=jnp.float32), approximate=False).astype(jnp.bfloat16)
    update = project_out(hidden, second_matrix).reshape(spatial.shape)
    return (state_wide + update).astype(jnp.bfloat16)

def reference(analysis, perturbations, gain_first, spectral_gain, skip_weight, gain_second, mlp_in, mlp_out):
    legendre, weights = legendre_table(NLAT, LMAX, MMAX, NLON, 0, MMAX)
    weighted = (legendre * weights[:, None, None]).astype(jnp.bfloat16)
    plain_table = legendre.astype(jnp.bfloat16)
    forward, inverse = fourier_tables(NLON, MMAX)
    pert_wide = perturbations.astype(jnp.float32)
    current_state = (analysis.astype(jnp.float32)[None] + pert_wide - lax.optimization_barrier(jnp.mean(pert_wide, axis=0, keepdims=True))).astype(jnp.bfloat16)
    outputs = []
    for block_index in range(N_SECTION):
        current_state = sfno_block(current_state, gain_first[block_index], spectral_gain[block_index], skip_weight[block_index], gain_second[block_index], mlp_in[block_index], mlp_out[block_index], weighted, plain_table, forward, inverse)
        outputs.append(current_state.reshape(MEMBERS, NLAT, NLON * C))
    return jnp.stack(outputs)
```

```python
import math

import jax
import jax.numpy as jnp
import numpy as np
from jax import lax
from jax.experimental import pallas as pl
from jax.experimental.pallas import tpu as pltpu
from jax.sharding import PartitionSpec as P

C = 192
NLAT = 128
NLON = 256
LMAX = 128
MMAX = 128


def shifted_2(value, axis, steps):
    count = lax.axis_size(axis)
    first, last = (max(0, -steps), min(count, count - steps))
    return lax.ppermute(value, axis, [(source, source + steps) for source in range(first, last)])


def legendre_kernel(cos_ref, diag_ref, order_ref, lower_ref, upper_ref, out_ref):
    cosine = cos_ref[...]
    diagonal = diag_ref[...]
    order = order_ref[...]
    first_step = jnp.sqrt(2.0 * order + 3.0) * cosine * diagonal

    def advance(degree, carry):
        latest, earlier = carry
        recurred = lower_ref[degree] * (cosine * latest - upper_ref[degree] * earlier)
        above = degree.astype(jnp.float32) - order
        current = jnp.where(
            above == 0.0,
            diagonal,
            jnp.where(above == 1.0, first_step, jnp.where(above > 1.0, recurred, 0.0)),
        )
        out_ref[degree] = current
        return (current, latest)

    initial = cosine * 0.0
    lax.fori_loop(0, out_ref.shape[0], advance, (initial, initial), unroll=8)


def legendre_table(nlat, lmax, mmax, nlon, m_first, m_count):
    colatitude = math.pi * (np.arange(nlat, dtype=np.float32) + np.float32(0.5)) / nlat
    colatitude = colatitude.astype(np.float32)
    cosine = np.cos(colatitude)
    sine = np.sin(colatitude)
    orders = np.arange(1, mmax, dtype=np.float64)
    factors = np.cumsum(0.5 * np.log((2.0 * orders + 1.0) / (2.0 * orders)))
    log_diag = np.concatenate([np.zeros((1,)), factors]).astype(np.float32)
    m_all = np.arange(mmax, dtype=np.float64)
    l_all = np.arange(lmax, dtype=np.float64)[:, None]
    lower_all = np.sqrt((4.0 * l_all * l_all - 1.0).clip(0.0) / np.maximum(l_all**2 - m_all**2, 1.0))
    shifted = l_all - 1.0
    upper_all = np.sqrt(
        np.maximum(shifted**2 - m_all**2, 0.0) / np.maximum(4.0 * shifted**2 - 1.0, 1.0)
    )
    packed = np.concatenate([lower_all, upper_all, log_diag[None], m_all[None]]).astype(np.float32)
    mine = lax.dynamic_slice_in_dim(jnp.asarray(packed), m_first, m_count, 1)
    lower, upper = (mine[:lmax], mine[lmax : 2 * lmax])
    picked, m_float = (mine[2 * lmax], mine[2 * lmax + 1])
    diagonal = jnp.exp(
        picked[:, None] + m_float[:, None] * jnp.asarray(np.log(sine))[None, :]
    ) * math.sqrt(0.25 / math.pi)
    wide = (m_count, nlat)
    legendre = pl.pallas_call(
        legendre_kernel,
        out_shape=jax.ShapeDtypeStruct((lmax,) + wide, jnp.float32),
        name="legendre",
    )(
        jnp.broadcast_to(jnp.asarray(cosine)[None, :], wide),
        diagonal,
        jnp.broadcast_to(m_float[:, None], wide),
        jnp.broadcast_to(lower[:, :, None], (lmax,) + wide),
        jnp.broadcast_to(upper[:, :, None], (lmax,) + wide),
    )
    weights = jnp.asarray(sine * np.float32(2.0 * math.pi / nlon) * np.float32(math.pi / nlat))
    return (legendre, weights)


def fourier_tables(nlon, mmax):
    samples = np.arange(nlon)
    orders = np.arange(mmax)
    phase = (samples[:, None] * orders[None, :] % nlon).astype(np.float64) * (2.0 * math.pi / nlon)
    cosines = np.cos(phase)
    sines = np.sin(phase)
    forward = np.stack([cosines, -sines], axis=1).astype(jnp.bfloat16)
    factor = np.where(orders == 0, 1.0, 2.0)
    inverse = np.stack([cosines.T * factor[:, None], -sines.T * factor[:, None]], axis=0)
    return (jnp.asarray(forward), jnp.asarray(inverse.astype(jnp.bfloat16)))


def layer_norm(values, gain_vector):
    average = jnp.mean(values, axis=-1, keepdims=True)
    centred = values - average
    variance = jnp.mean(centred * centred, axis=-1, keepdims=True)
    return centred * lax.rsqrt(variance + 1e-05) * gain_vector


def apply_gain(coeffs, gain_table):
    real_part = coeffs[:, :, :, 0]
    imag_part = coeffs[:, :, :, 1]
    gain_real = gain_table[0][None, :, None, :]
    gain_imag = gain_table[1][None, :, None, :]
    return jnp.stack(
        [
            real_part * gain_real - imag_part * gain_imag,
            real_part * gain_imag + imag_part * gain_real,
        ],
        axis=3,
    )


def recenter(analysis, perturbations):
    pert_wide = perturbations.astype(jnp.float32)
    average = jnp.mean(pert_wide, axis=0, keepdims=True)
    return (analysis.astype(jnp.float32)[None] + pert_wide - average).astype(jnp.bfloat16)


def project_out(hidden, out_matrix):
    return lax.dot_general(
        hidden, out_matrix, (((1,), (1,)), ((), ())), preferred_element_type=jnp.float32
    )


def make_block(m_count, tables):
    forward, inverse, weighted, plain_table = tables

    def spectral(normed, full_gain):
        batch_rows = normed.shape[0]
        lat_rows = normed.shape[1]
        spectrum = jnp.einsum(
            "bjkc,kpm->bjmpc", normed, forward, preferred_element_type=jnp.float32
        ).astype(jnp.bfloat16)
        spectrum = spectrum.reshape(batch_rows, lat_rows, MMAX, 2 * C)
        exchanged = lax.all_to_all(spectrum, "sht", split_axis=2, concat_axis=1, tiled=True)
        item_count = exchanged.shape[0]
        coeffs = jnp.einsum(
            "lmj,bjmq->blmq", weighted, exchanged, preferred_element_type=jnp.float32
        )
        coeffs = coeffs.reshape(item_count, LMAX, m_count, 2, C)
        filtered = (
            apply_gain(coeffs, full_gain)
            .astype(jnp.bfloat16)
            .reshape(item_count, LMAX, m_count, 2 * C)
        )
        returned = jnp.einsum(
            "lmj,blmq->bjmq", plain_table, filtered, preferred_element_type=jnp.float32
        ).astype(jnp.bfloat16)
        returned = lax.all_to_all(returned, "sht", split_axis=1, concat_axis=2, tiled=True)
        returned = returned.reshape(batch_rows, lat_rows, MMAX, 2, C)
        return jnp.einsum("bjmpc,pmk->bjkc", returned, inverse, preferred_element_type=jnp.float32)

    def sfno_block(current_state, params):
        gain_one, full_gain, skip_matrix, gain_two, first_matrix, second_matrix = params
        state_wide = current_state.astype(jnp.float32)
        channels = current_state.shape[-1]
        normed = layer_norm(state_wide, gain_one).astype(jnp.bfloat16)
        spatial = spectral(normed, full_gain)
        skipped = jnp.dot(
            normed.reshape(-1, channels), skip_matrix, preferred_element_type=jnp.float32
        ).reshape(spatial.shape)
        activated = jax.nn.gelu(spatial + skipped, approximate=False)
        second = layer_norm(activated, gain_two).astype(jnp.bfloat16)
        hidden = jax.nn.gelu(
            jnp.dot(second.reshape(-1, channels), first_matrix, preferred_element_type=jnp.float32),
            approximate=False,
        ).astype(jnp.bfloat16)
        update = project_out(hidden, second_matrix).reshape(spatial.shape)
        return (state_wide + update).astype(jnp.bfloat16)

    return sfno_block


def piped(centred, own_params, sfno_block):
    section_index = lax.axis_index("section")
    section_count = lax.axis_size("section")
    members = lax.all_gather(centred, "section", axis=3, tiled=True)
    batch_count = members.shape[0]

    def tick(tick_index, carry):
        current_state, stored = carry
        received = shifted_2(current_state, "section", 1)
        first_rows = lax.dynamic_slice_in_dim(
            members, jnp.minimum(tick_index, batch_count - 1), 1, 0
        )
        incoming = jnp.where(section_index == 0, first_rows, received)
        result = sfno_block(incoming, own_params)
        position = tick_index - section_index
        is_valid = jnp.logical_and(position >= 0, position < batch_count)
        offset = jnp.clip(position, 0, batch_count - 1)
        previous = lax.dynamic_slice_in_dim(stored, offset, 1, 0)
        stored = lax.dynamic_update_slice_in_dim(
            stored, jnp.where(is_valid, result, previous), offset, 0
        )
        return (result, stored)

    empty_state = jnp.zeros((1,) + members.shape[1:], jnp.bfloat16)
    _, stored = lax.fori_loop(
        0, section_count + batch_count - 1, tick, (empty_state, jnp.zeros_like(members))
    )
    merged = stored.reshape(stored.shape[0], stored.shape[1], stored.shape[2] * stored.shape[3])
    return merged[None]


def swapped(value):
    return lax.ppermute(value, "section", [(0, 1), (1, 0)])


def split(centred, own_params, sfno_block):
    is_first = lax.axis_index("section") == 0
    half = centred.shape[0] // 2

    def both_blocks(value):
        other = swapped(value)
        return (jnp.where(is_first, value, other), jnp.where(is_first, other, value))

    gain_one, full_gain, skip_matrix, gain_two, first_matrix, second_matrix = own_params
    channels = skip_matrix.shape[0]
    hidden_units = first_matrix.shape[1]
    narrow = both_blocks(jnp.concatenate([skip_matrix, first_matrix, second_matrix], axis=1))
    wide = both_blocks(
        jnp.concatenate([gain_one[None], gain_two[None], full_gain.reshape(-1, channels)], axis=0)
    )
    params = [
        (
            wide[b][0],
            wide[b][2:].reshape(full_gain.shape),
            narrow[b][:, :channels],
            wide[b][1],
            narrow[b][:, channels : channels + hidden_units],
            narrow[b][:, channels + hidden_units :],
        )
        for b in range(2)
    ]
    head, tail = ([], [])
    for index in range(half):
        low, high = (centred[index], centred[half + index])
        kept = jnp.where(is_first, low, high)
        arrived = swapped(jnp.where(is_first, high, low))
        state = jnp.concatenate(
            [jnp.where(is_first, kept, arrived), jnp.where(is_first, arrived, kept)], axis=-1
        )[None]
        first = sfno_block(state, params[0])
        second = sfno_block(first, params[1])
        first_flat = first.reshape(first.shape[1], -1)
        second_flat = second.reshape(second.shape[1], -1)
        first_there = lax.ppermute(first_flat, "section", [(1, 0)])
        second_there = lax.ppermute(second_flat, "section", [(0, 1)])
        head.append(jnp.where(is_first, first_flat, second_there))
        tail.append(jnp.where(is_first, first_there, second_flat))
    return jnp.stack(head + tail)[None]


def per_device(
    analysis, perturbations, gain_first, spectral_gain, skip_weight, gain_second, mlp_in, mlp_out
):
    centred = recenter(analysis, perturbations)
    forward, inverse = fourier_tables(NLON, MMAX)
    m_count = MMAX // lax.axis_size("sht")
    legendre, weights = legendre_table(
        NLAT, LMAX, MMAX, NLON, lax.axis_index("sht") * m_count, m_count
    )
    weighted = (legendre * weights).astype(jnp.bfloat16)
    plain_table = legendre.astype(jnp.bfloat16)
    block = make_block(m_count, (forward, inverse, weighted, plain_table))
    own_params = (
        gain_first[0],
        spectral_gain[0].reshape(2, LMAX, C),
        skip_weight[0],
        gain_second[0],
        mlp_in[0],
        mlp_out[0],
    )
    if lax.axis_size("section") == 2 and centred.shape[0] % 2 == 0:
        return split(centred, own_params, block)
    return piped(centred, own_params, block)


def solution(mesh):
    return jax.shard_map(
        per_device,
        mesh=mesh,
        in_specs=(
            P("sht", None, "section"),
            P(None, "sht", None, "section"),
            P("section", None),
            P("section", None, None),
            P("section", None, None),
            P("section", None),
            P("section", None, None),
            P("section", None, None),
        ),
        out_specs=P("section", None, "sht", None),
        check_vma=False,
    )
```

```python
import math

import jax
import jax.numpy as jnp
import numpy as np
from jax import lax
from jax.experimental import pallas as pl
from jax.experimental.pallas import tpu as pltpu
from jax.sharding import PartitionSpec as P

C = 192
NLAT = 128
NLON = 256
LMAX = 128
MMAX = 128


def shifted_2(value, axis, steps):
    count = lax.axis_size(axis)
    first, last = (max(0, -steps), min(count, count - steps))
    return lax.ppermute(value, axis, [(source, source + steps) for source in range(first, last)])


def legendre_kernel(cos_ref, diag_ref, order_ref, lower_ref, upper_ref, out_ref):
    cosine = cos_ref[...]
    diagonal = diag_ref[...]
    order = order_ref[...]
    first_step = jnp.sqrt(2.0 * order + 3.0) * cosine * diagonal

    def advance(degree, carry):
        latest, earlier = carry
        recurred = lower_ref[degree] * (cosine * latest - upper_ref[degree] * earlier)
        above = degree.astype(jnp.float32) - order
        current = jnp.where(
            above == 0.0,
            diagonal,
            jnp.where(above == 1.0, first_step, jnp.where(above > 1.0, recurred, 0.0)),
        )
        out_ref[degree] = current
        return (current, latest)

    initial = cosine * 0.0
    lax.fori_loop(0, out_ref.shape[0], advance, (initial, initial), unroll=8)


def legendre_table(nlat, lmax, mmax, nlon, m_first, m_count):
    colatitude = math.pi * (np.arange(nlat, dtype=np.float32) + np.float32(0.5)) / nlat
    colatitude = colatitude.astype(np.float32)
    cosine = np.cos(colatitude)
    sine = np.sin(colatitude)
    orders = np.arange(1, mmax, dtype=np.float64)
    factors = np.cumsum(0.5 * np.log((2.0 * orders + 1.0) / (2.0 * orders)))
    log_diag = np.concatenate([np.zeros((1,)), factors]).astype(np.float32)
    m_all = np.arange(mmax, dtype=np.float64)
    l_all = np.arange(lmax, dtype=np.float64)[:, None]
    lower_all = np.sqrt((4.0 * l_all * l_all - 1.0).clip(0.0) / np.maximum(l_all**2 - m_all**2, 1.0))
    shifted = l_all - 1.0
    upper_all = np.sqrt(
        np.maximum(shifted**2 - m_all**2, 0.0) / np.maximum(4.0 * shifted**2 - 1.0, 1.0)
    )
    packed = np.concatenate([lower_all, upper_all, log_diag[None], m_all[None]]).astype(np.float32)
    mine = lax.dynamic_slice_in_dim(jnp.asarray(packed), m_first, m_count, 1)
    lower, upper = (mine[:lmax], mine[lmax : 2 * lmax])
    picked, m_float = (mine[2 * lmax], mine[2 * lmax + 1])
    diagonal = jnp.exp(
        picked[:, None] + m_float[:, None] * jnp.asarray(np.log(sine))[None, :]
    ) * math.sqrt(0.25 / math.pi)
    wide = (m_count, nlat)
    legendre = pl.pallas_call(
        legendre_kernel,
        out_shape=jax.ShapeDtypeStruct((lmax,) + wide, jnp.float32),
        name="legendre",
    )(
        jnp.broadcast_to(jnp.asarray(cosine)[None, :], wide),
        diagonal,
        jnp.broadcast_to(m_float[:, None], wide),
        jnp.broadcast_to(lower[:, :, None], (lmax,) + wide),
        jnp.broadcast_to(upper[:, :, None], (lmax,) + wide),
    )
    weights = jnp.asarray(sine * np.float32(2.0 * math.pi / nlon) * np.float32(math.pi / nlat))
    return (legendre, weights)


def fourier_tables(nlon, mmax):
    samples = np.arange(nlon)
    orders = np.arange(mmax)
    phase = (samples[:, None] * orders[None, :] % nlon).astype(np.float64) * (2.0 * math.pi / nlon)
    cosines = np.cos(phase)
    sines = np.sin(phase)
    forward = np.stack([cosines, -sines], axis=1).astype(jnp.bfloat16)
    factor = np.where(orders == 0, 1.0, 2.0)
    inverse = np.stack([cosines.T * factor[:, None], -sines.T * factor[:, None]], axis=0)
    return (jnp.asarray(forward), jnp.asarray(inverse.astype(jnp.bfloat16)))


def layer_norm(values, gain_vector):
    average = jnp.mean(values, axis=-1, keepdims=True)
    centred = values - average
    variance = jnp.mean(centred * centred, axis=-1, keepdims=True)
    return centred * lax.rsqrt(variance + 1e-05) * gain_vector


def apply_gain(coeffs, gain_table):
    real_part = coeffs[:, :, :, 0]
    imag_part = coeffs[:, :, :, 1]
    gain_real = gain_table[0][None, :, None, :]
    gain_imag = gain_table[1][None, :, None, :]
    return jnp.stack(
        [
            real_part * gain_real - imag_part * gain_imag,
            real_part * gain_imag + imag_part * gain_real,
        ],
        axis=3,
    )


def recenter(analysis, perturbations):
    pert_wide = perturbations.astype(jnp.float32)
    average = jnp.mean(pert_wide, axis=0, keepdims=True)
    return (analysis.astype(jnp.float32)[None] + pert_wide - average).astype(jnp.bfloat16)


def project_out(hidden, out_matrix):
    return lax.dot_general(
        hidden, out_matrix, (((1,), (1,)), ((), ())), preferred_element_type=jnp.float32
    )


def make_block(m_count, tables):
    forward, inverse, weighted, plain_table = tables

    def spectral(normed, full_gain):
        batch_rows = normed.shape[0]
        lat_rows = normed.shape[1]
        spectrum = jnp.einsum(
            "bjkc,kpm->bjmpc", normed, forward, preferred_element_type=jnp.float32
        ).astype(jnp.bfloat16)
        spectrum = spectrum.reshape(batch_rows, lat_rows, MMAX, 2 * C)
        exchanged = lax.all_to_all(spectrum, "sht", split_axis=2, concat_axis=1, tiled=True)
        item_count = exchanged.shape[0]
        coeffs = jnp.einsum(
            "lmj,bjmq->blmq", weighted, exchanged, preferred_element_type=jnp.float32
        )
        coeffs = coeffs.reshape(item_count, LMAX, m_count, 2, C)
        filtered = (
            apply_gain(coeffs, full_gain)
            .astype(jnp.bfloat16)
            .reshape(item_count, LMAX, m_count, 2 * C)
        )
        returned = jnp.einsum(
            "lmj,blmq->bjmq", plain_table, filtered, preferred_element_type=jnp.float32
        ).astype(jnp.bfloat16)
        returned = lax.all_to_all(returned, "sht", split_axis=1, concat_axis=2, tiled=True)
        returned = returned.reshape(batch_rows, lat_rows, MMAX, 2, C)
        return jnp.einsum("bjmpc,pmk->bjkc", returned, inverse, preferred_element_type=jnp.float32)

    def sfno_block(current_state, params):
        gain_one, full_gain, skip_matrix, gain_two, first_matrix, second_matrix = params
        state_wide = current_state.astype(jnp.float32)
        channels = current_state.shape[-1]
        normed = layer_norm(state_wide, gain_one).astype(jnp.bfloat16)
        spatial = spectral(normed, full_gain)
        skipped = jnp.dot(
            normed.reshape(-1, channels), skip_matrix, preferred_element_type=jnp.float32
        ).reshape(spatial.shape)
        activated = jax.nn.gelu(spatial + skipped, approximate=False)
        second = layer_norm(activated, gain_two).astype(jnp.bfloat16)
        hidden = jax.nn.gelu(
            jnp.dot(second.reshape(-1, channels), first_matrix, preferred_element_type=jnp.float32),
            approximate=False,
        ).astype(jnp.bfloat16)
        update = project_out(hidden, second_matrix).reshape(spatial.shape)
        return (state_wide + update).astype(jnp.bfloat16)

    return sfno_block


def piped(centred, own_params, sfno_block):
    section_index = lax.axis_index("section")
    section_count = lax.axis_size("section")
    members = lax.all_gather(centred, "section", axis=3, tiled=True)
    batch_count = members.shape[0]

    def tick(tick_index, carry):
        current_state, stored = carry
        received = shifted_2(current_state, "section", 1)
        first_rows = lax.dynamic_slice_in_dim(
            members, jnp.minimum(tick_index, batch_count - 1), 1, 0
        )
        incoming = jnp.where(section_index == 0, first_rows, received)
        result = sfno_block(incoming, own_params)
        position = tick_index - section_index
        is_valid = jnp.logical_and(position >= 0, position < batch_count)
        offset = jnp.clip(position, 0, batch_count - 1)
        previous = lax.dynamic_slice_in_dim(stored, offset, 1, 0)
        stored = lax.dynamic_update_slice_in_dim(
            stored, jnp.where(is_valid, result, previous), offset, 0
        )
        return (result, stored)

    empty_state = jnp.zeros((1,) + members.shape[1:], jnp.bfloat16)
    _, stored = lax.fori_loop(
        0, section_count + batch_count - 1, tick, (empty_state, jnp.zeros_like(members))
    )
    merged = stored.reshape(stored.shape[0], stored.shape[1], stored.shape[2] * stored.shape[3])
    return merged[None]


def row_norm(values, gain_row):
    average = jnp.mean(values, axis=1, keepdims=True)
    centred = values - average
    variance = jnp.mean(centred * centred, axis=1, keepdims=True)
    return (centred * lax.rsqrt(variance + 1e-05) * gain_row).astype(jnp.bfloat16)


def wide_dot(left, right):
    return jnp.dot(left, right, preferred_element_type=jnp.float32)


def exact_gelu(values):
    return 0.5 * values * (1.0 + lax.erf(values * math.sqrt(0.5)))


def row_spectrum(normed, forward_ref):
    return jnp.concatenate(
        [wide_dot(forward_ref[0], normed), wide_dot(forward_ref[1], normed)], axis=1
    ).astype(jnp.bfloat16)


def pre_kernel(state_ref, gain_ref, forward_ref, spectrum_ref):
    normed = row_norm(state_ref[0].astype(jnp.float32), gain_ref[...])
    spectrum_ref[0] = row_spectrum(normed, forward_ref)


def post_kernel(
    returned_ref, state_ref, inverse_ref, forward_ref, gain_one_ref, gain_two_ref, gain_next_ref,
    skip_ref, first_ref, second_ref, result_ref, *spectrum_refs
):
    channels = state_ref.shape[2]
    state = state_ref[0].astype(jnp.float32)
    normed = row_norm(state, gain_one_ref[...])
    returned = returned_ref[0]
    spatial = wide_dot(inverse_ref[0], returned[:, :channels])
    spatial = spatial + wide_dot(inverse_ref[1], returned[:, channels:])
    activated = exact_gelu(spatial + wide_dot(normed, skip_ref[...]))
    second = row_norm(activated, gain_two_ref[...])
    hidden = exact_gelu(wide_dot(second, first_ref[...])).astype(jnp.bfloat16)
    result = (state + wide_dot(hidden, second_ref[...])).astype(jnp.bfloat16)
    result_ref[0] = result
    for spectrum_ref in spectrum_refs:
        following = row_norm(result.astype(jnp.float32), gain_next_ref[...])
        spectrum_ref[0] = row_spectrum(following, forward_ref)


def by_row(shape):
    return pl.BlockSpec((1,) + tuple(shape[1:]), lambda row: (row, 0, 0))


def held(value):
    return pl.BlockSpec(value.shape, lambda row: (0,) * value.ndim)


def call_pre(state, gain, forward):
    lats, lons, channels = state.shape
    spectrum = jax.ShapeDtypeStruct((lats, forward.shape[1], 2 * channels), jnp.bfloat16)
    return pl.pallas_call(
        pre_kernel,
        grid=(lats,),
        in_specs=[by_row(state.shape), held(gain), held(forward)],
        out_specs=by_row(spectrum.shape),
        out_shape=spectrum,
        cost_estimate=pl.CostEstimate(
            flops=4 * state.size * forward.shape[1], bytes_accessed=4 * state.size, transcendentals=0
        ),
        name="pre",
    )(state, gain, forward)


def call_post(returned, state, inverse, forward, params, gain_next):
    gain_one, gain_two, skip, first, second = params
    lats, lons, channels = state.shape
    weights = [inverse, forward, gain_one, gain_two]
    weights += [gain_one if gain_next is None else gain_next, skip, first, second]
    shapes = [jax.ShapeDtypeStruct(state.shape, jnp.bfloat16)]
    if gain_next is not None:
        shapes.append(jax.ShapeDtypeStruct(returned.shape, jnp.bfloat16))
    flops = 2 * state.size * (4 * forward.shape[1] + channels + 2 * first.shape[1])
    return pl.pallas_call(
        post_kernel,
        grid=(lats,),
        in_specs=[by_row(returned.shape), by_row(state.shape)] + [held(w) for w in weights],
        out_specs=[by_row(shape.shape) for shape in shapes],
        out_shape=shapes,
        cost_estimate=pl.CostEstimate(
            flops=4 * flops, bytes_accessed=8 * state.size, transcendentals=3 * state.size
        ),
        name="post",
    )(returned, state, *weights)


def swapped(value):
    return lax.ppermute(value, "section", [(0, 1), (1, 0)])


def split(centred, own_params, tables):
    is_first = lax.axis_index("section") == 0
    half = centred.shape[0] // 2
    forward, inverse, weighted, plain_table = tables
    forward_rows = jnp.transpose(forward, (1, 2, 0))
    inverse_rows = jnp.transpose(inverse, (0, 2, 1))

    def sides(value, other):
        return (jnp.where(is_first, value, other), jnp.where(is_first, other, value))

    gain_one, full_gain, skip_matrix, gain_two, first_matrix, second_matrix = own_params
    channels = skip_matrix.shape[0]
    hidden_units = first_matrix.shape[1]
    m_count = weighted.shape[1]
    states = []
    own_gain = jnp.pad(jnp.stack([gain_one, gain_two]), ((0, 6), (0, 0)))
    gains = sides(own_gain, swapped(own_gain))
    for index in range(half):
        low, high = (centred[index], centred[half + index])
        kept = jnp.where(is_first, low, high)
        arrived = swapped(jnp.where(is_first, high, low))
        states.append(jnp.concatenate(sides(kept, arrived), axis=-1))
    own_narrow = jnp.concatenate([skip_matrix, first_matrix, second_matrix], axis=1)
    own_filter = full_gain.reshape(-1, channels)
    narrow_there = swapped(own_narrow)
    filter_there = swapped(own_filter)

    def outward(spectrum):
        return lax.all_to_all(spectrum[None], "sht", split_axis=2, concat_axis=1, tiled=True)

    def middle(exchanged, filter_table):
        coeffs = jnp.einsum(
            "lmj,bjmq->blmq", weighted, exchanged, preferred_element_type=jnp.float32
        ).reshape(1, LMAX, m_count, 2, channels)
        filtered = apply_gain(coeffs, filter_table).astype(jnp.bfloat16)
        filtered = filtered.reshape(1, LMAX, m_count, 2 * channels)
        returned = jnp.einsum(
            "lmj,blmq->bjmq", plain_table, filtered, preferred_element_type=jnp.float32
        ).astype(jnp.bfloat16)
        return lax.all_to_all(returned, "sht", split_axis=1, concat_axis=2, tiled=True)[0]

    exchanged = [outward(call_pre(state, gains[0][0:1], forward_rows)) for state in states]
    exchanged[0], narrow_there, filter_there = lax.optimization_barrier(
        (exchanged[0], narrow_there, filter_there)
    )
    narrow = sides(own_narrow, narrow_there)
    filters = [f.reshape(full_gain.shape) for f in sides(own_filter, filter_there)]
    params = [
        (
            gains[b][0:1],
            gains[b][1:2],
            narrow[b][:, :channels],
            narrow[b][:, channels : channels + hidden_units],
            jnp.transpose(narrow[b][:, channels + hidden_units :]),
        )
        for b in range(2)
    ]
    returned = [middle(one, filters[0]) for one in exchanged]
    between = [
        call_post(one, state, inverse_rows, forward_rows, params[0], gains[1][0:1])
        for one, state in zip(returned, states)
    ]
    flats = [state.reshape(state.shape[0], -1) for state, _ in between]
    first_there = [lax.ppermute(flat, "section", [(1, 0)]) for flat in flats]
    exchanged = [outward(spectrum) for _, spectrum in between]
    returned = [middle(one, filters[1]) for one in exchanged]
    head, tail = ([], [])
    for index in range(half):
        back, there = lax.optimization_barrier((returned[index], first_there[index]))
        (last,) = call_post(back, between[index][0], inverse_rows, forward_rows, params[1], None)
        flat = last.reshape(last.shape[0], -1)
        head.append(jnp.where(is_first, flats[index], lax.ppermute(flat, "section", [(0, 1)])))
        tail.append(jnp.where(is_first, there, flat))
    return jnp.stack(head + tail)[None]


def per_device(
    analysis, perturbations, gain_first, spectral_gain, skip_weight, gain_second, mlp_in, mlp_out
):
    centred = recenter(analysis, perturbations)
    forward, inverse = fourier_tables(NLON, MMAX)
    m_count = MMAX // lax.axis_size("sht")
    legendre, weights = legendre_table(
        NLAT, LMAX, MMAX, NLON, lax.axis_index("sht") * m_count, m_count
    )
    weighted = (legendre * weights).astype(jnp.bfloat16)
    plain_table = legendre.astype(jnp.bfloat16)
    block = make_block(m_count, (forward, inverse, weighted, plain_table))
    own_params = (
        gain_first[0],
        spectral_gain[0].reshape(2, LMAX, C),
        skip_weight[0],
        gain_second[0],
        mlp_in[0],
        mlp_out[0],
    )
    if lax.axis_size("section") == 2 and centred.shape[0] % 2 == 0:
        return split(centred, own_params, (forward, inverse, weighted, plain_table))
    return piped(centred, own_params, block)


def solution(mesh):
    return jax.shard_map(
        per_device,
        mesh=mesh,
        in_specs=(
            P("sht", None, "section"),
            P(None, "sht", None, "section"),
            P("section", None),
            P("section", None, None),
            P("section", None, None),
            P("section", None),
            P("section", None, None),
            P("section", None, None),
        ),
        out_specs=P("section", None, "sht", None),
        check_vma=False,
    )
```

```python
import math

import jax
import jax.numpy as jnp
import numpy as np
from jax import lax
from jax.experimental import pallas as pl
from jax.experimental.pallas import tpu as pltpu
from jax.sharding import PartitionSpec as P

C = 192
NLAT = 128
NLON = 256
LMAX = 128
MMAX = 128


def shifted_2(value, axis, steps):
    count = lax.axis_size(axis)
    first, last = (max(0, -steps), min(count, count - steps))
    return lax.ppermute(value, axis, [(source, source + steps) for source in range(first, last)])


def legendre_kernel(cos_ref, diag_ref, order_ref, lower_ref, upper_ref, out_ref):
    cosine = cos_ref[...]
    diagonal = diag_ref[...]
    order = order_ref[...]
    first_step = jnp.sqrt(2.0 * order + 3.0) * cosine * diagonal

    def advance(degree, carry):
        latest, earlier = carry
        recurred = lower_ref[degree] * (cosine * latest - upper_ref[degree] * earlier)
        above = degree.astype(jnp.float32) - order
        current = jnp.where(
            above == 0.0,
            diagonal,
            jnp.where(above == 1.0, first_step, jnp.where(above > 1.0, recurred, 0.0)),
        )
        out_ref[degree] = current
        return (current, latest)

    initial = cosine * 0.0
    lax.fori_loop(0, out_ref.shape[0], advance, (initial, initial), unroll=8)


def legendre_table(nlat, lmax, mmax, nlon, m_first, m_count):
    colatitude = math.pi * (np.arange(nlat, dtype=np.float32) + np.float32(0.5)) / nlat
    colatitude = colatitude.astype(np.float32)
    cosine = np.cos(colatitude)
    sine = np.sin(colatitude)
    orders = np.arange(1, mmax, dtype=np.float64)
    factors = np.cumsum(0.5 * np.log((2.0 * orders + 1.0) / (2.0 * orders)))
    log_diag = np.concatenate([np.zeros((1,)), factors]).astype(np.float32)
    m_all = np.arange(mmax, dtype=np.float64)
    l_all = np.arange(lmax, dtype=np.float64)[:, None]
    lower_all = np.sqrt((4.0 * l_all * l_all - 1.0).clip(0.0) / np.maximum(l_all**2 - m_all**2, 1.0))
    shifted = l_all - 1.0
    upper_all = np.sqrt(
        np.maximum(shifted**2 - m_all**2, 0.0) / np.maximum(4.0 * shifted**2 - 1.0, 1.0)
    )
    packed = np.concatenate([lower_all, upper_all, log_diag[None], m_all[None]]).astype(np.float32)
    mine = lax.dynamic_slice_in_dim(jnp.asarray(packed), m_first, m_count, 1)
    lower, upper = (mine[:lmax], mine[lmax : 2 * lmax])
    picked, m_float = (mine[2 * lmax], mine[2 * lmax + 1])
    diagonal = jnp.exp(
        picked[:, None] + m_float[:, None] * jnp.asarray(np.log(sine))[None, :]
    ) * math.sqrt(0.25 / math.pi)
    wide = (m_count, nlat)
    legendre = pl.pallas_call(
        legendre_kernel,
        out_shape=jax.ShapeDtypeStruct((lmax,) + wide, jnp.float32),
        name="legendre",
    )(
        jnp.broadcast_to(jnp.asarray(cosine)[None, :], wide),
        diagonal,
        jnp.broadcast_to(m_float[:, None], wide),
        jnp.broadcast_to(lower[:, :, None], (lmax,) + wide),
        jnp.broadcast_to(upper[:, :, None], (lmax,) + wide),
    )
    weights = jnp.asarray(sine * np.float32(2.0 * math.pi / nlon) * np.float32(math.pi / nlat))
    return (legendre, weights)


def fourier_tables(nlon, mmax):
    samples = np.arange(nlon)
    orders = np.arange(mmax)
    phase = (samples[:, None] * orders[None, :] % nlon).astype(np.float64) * (2.0 * math.pi / nlon)
    cosines = np.cos(phase)
    sines = np.sin(phase)
    forward = np.stack([cosines, -sines], axis=1).astype(jnp.bfloat16)
    factor = np.where(orders == 0, 1.0, 2.0)
    inverse = np.stack([cosines.T * factor[:, None], -sines.T * factor[:, None]], axis=0)
    return (jnp.asarray(forward), jnp.asarray(inverse.astype(jnp.bfloat16)))


def layer_norm(values, gain_vector):
    average = jnp.mean(values, axis=-1, keepdims=True)
    centred = values - average
    variance = jnp.mean(centred * centred, axis=-1, keepdims=True)
    return centred * lax.rsqrt(variance + 1e-05) * gain_vector


def apply_gain(coeffs, gain_table):
    real_part = coeffs[:, :, :, 0]
    imag_part = coeffs[:, :, :, 1]
    gain_real = gain_table[0][None, :, None, :]
    gain_imag = gain_table[1][None, :, None, :]
    return jnp.stack(
        [
            real_part * gain_real - imag_part * gain_imag,
            real_part * gain_imag + imag_part * gain_real,
        ],
        axis=3,
    )


def recenter(analysis, perturbations):
    pert_wide = perturbations.astype(jnp.float32)
    average = jnp.mean(pert_wide, axis=0, keepdims=True)
    return (analysis.astype(jnp.float32)[None] + pert_wide - average).astype(jnp.bfloat16)


def project_out(hidden, out_matrix):
    return lax.dot_general(
        hidden, out_matrix, (((1,), (1,)), ((), ())), preferred_element_type=jnp.float32
    )


def make_block(m_count, tables):
    forward, inverse, weighted, plain_table = tables

    def spectral(normed, full_gain):
        batch_rows = normed.shape[0]
        lat_rows = normed.shape[1]
        spectrum = jnp.einsum(
            "bjkc,kpm->bjmpc", normed, forward, preferred_element_type=jnp.float32
        ).astype(jnp.bfloat16)
        spectrum = spectrum.reshape(batch_rows, lat_rows, MMAX, 2 * C)
        exchanged = lax.all_to_all(spectrum, "sht", split_axis=2, concat_axis=1, tiled=True)
        item_count = exchanged.shape[0]
        coeffs = jnp.einsum(
            "lmj,bjmq->blmq", weighted, exchanged, preferred_element_type=jnp.float32
        )
        coeffs = coeffs.reshape(item_count, LMAX, m_count, 2, C)
        filtered = (
            apply_gain(coeffs, full_gain)
            .astype(jnp.bfloat16)
            .reshape(item_count, LMAX, m_count, 2 * C)
        )
        returned = jnp.einsum(
            "lmj,blmq->bjmq", plain_table, filtered, preferred_element_type=jnp.float32
        ).astype(jnp.bfloat16)
        returned = lax.all_to_all(returned, "sht", split_axis=1, concat_axis=2, tiled=True)
        returned = returned.reshape(batch_rows, lat_rows, MMAX, 2, C)
        return jnp.einsum("bjmpc,pmk->bjkc", returned, inverse, preferred_element_type=jnp.float32)

    def sfno_block(current_state, params):
        gain_one, full_gain, skip_matrix, gain_two, first_matrix, second_matrix = params
        state_wide = current_state.astype(jnp.float32)
        channels = current_state.shape[-1]
        normed = layer_norm(state_wide, gain_one).astype(jnp.bfloat16)
        spatial = spectral(normed, full_gain)
        skipped = jnp.dot(
            normed.reshape(-1, channels), skip_matrix, preferred_element_type=jnp.float32
        ).reshape(spatial.shape)
        activated = jax.nn.gelu(spatial + skipped, approximate=False)
        second = layer_norm(activated, gain_two).astype(jnp.bfloat16)
        hidden = jax.nn.gelu(
            jnp.dot(second.reshape(-1, channels), first_matrix, preferred_element_type=jnp.float32),
            approximate=False,
        ).astype(jnp.bfloat16)
        update = project_out(hidden, second_matrix).reshape(spatial.shape)
        return (state_wide + update).astype(jnp.bfloat16)

    return sfno_block


def piped(centred, own_params, sfno_block):
    section_index = lax.axis_index("section")
    section_count = lax.axis_size("section")
    members = lax.all_gather(centred, "section", axis=3, tiled=True)
    batch_count = members.shape[0]

    def tick(tick_index, carry):
        current_state, stored = carry
        received = shifted_2(current_state, "section", 1)
        first_rows = lax.dynamic_slice_in_dim(
            members, jnp.minimum(tick_index, batch_count - 1), 1, 0
        )
        incoming = jnp.where(section_index == 0, first_rows, received)
        result = sfno_block(incoming, own_params)
        position = tick_index - section_index
        is_valid = jnp.logical_and(position >= 0, position < batch_count)
        offset = jnp.clip(position, 0, batch_count - 1)
        previous = lax.dynamic_slice_in_dim(stored, offset, 1, 0)
        stored = lax.dynamic_update_slice_in_dim(
            stored, jnp.where(is_valid, result, previous), offset, 0
        )
        return (result, stored)

    empty_state = jnp.zeros((1,) + members.shape[1:], jnp.bfloat16)
    _, stored = lax.fori_loop(
        0, section_count + batch_count - 1, tick, (empty_state, jnp.zeros_like(members))
    )
    merged = stored.reshape(stored.shape[0], stored.shape[1], stored.shape[2] * stored.shape[3])
    return merged[None]


def row_norm(values, gain_row):
    average = jnp.mean(values, axis=1, keepdims=True)
    centred = values - average
    variance = jnp.mean(centred * centred, axis=1, keepdims=True)
    return (centred * lax.rsqrt(variance + 1e-05) * gain_row).astype(jnp.bfloat16)


def wide_dot(left, right):
    return jnp.dot(left, right, preferred_element_type=jnp.float32)


def exact_gelu(values):
    return 0.5 * values * (1.0 + lax.erf(values * math.sqrt(0.5)))


def row_spectrum(normed, forward_ref):
    return jnp.concatenate(
        [wide_dot(forward_ref[0], normed), wide_dot(forward_ref[1], normed)], axis=1
    ).astype(jnp.bfloat16)


def pre_kernel(first_ref, kept_ref, arrived_ref, gain_ref, forward_ref, state_ref, spectrum_ref):
    kept = kept_ref[0].astype(jnp.float32)
    arrived = arrived_ref[0].astype(jnp.float32)
    is_first = first_ref[0] == 1
    state = jnp.concatenate(
        [jnp.where(is_first, kept, arrived), jnp.where(is_first, arrived, kept)], axis=1
    )
    state_ref[0] = state.astype(jnp.bfloat16)
    normed = row_norm(state, gain_ref[...])
    spectrum_ref[0] = row_spectrum(normed, forward_ref)


def post_kernel(
    returned_ref, state_ref, inverse_ref, forward_ref, gain_one_ref, gain_two_ref, gain_next_ref,
    skip_ref, first_ref, second_ref, result_ref, *spectrum_refs
):
    channels = state_ref.shape[2]
    state = state_ref[0].astype(jnp.float32)
    normed = row_norm(state, gain_one_ref[...])
    returned = returned_ref[0]
    spatial = wide_dot(inverse_ref[0], returned[:, :channels])
    spatial = spatial + wide_dot(inverse_ref[1], returned[:, channels:])
    activated = exact_gelu(spatial + wide_dot(normed, skip_ref[...]))
    second = row_norm(activated, gain_two_ref[...])
    hidden = exact_gelu(wide_dot(second, first_ref[...])).astype(jnp.bfloat16)
    result = (state + wide_dot(hidden, second_ref[...])).astype(jnp.bfloat16)
    result_ref[0] = result
    for spectrum_ref in spectrum_refs:
        following = row_norm(result.astype(jnp.float32), gain_next_ref[...])
        spectrum_ref[0] = row_spectrum(following, forward_ref)


def by_row(shape):
    return pl.BlockSpec((1,) + tuple(shape[1:]), lambda row: (row, 0, 0))


def held(value):
    return pl.BlockSpec(value.shape, lambda row: (0,) * value.ndim)


def call_pre(is_first, kept, arrived, gain, forward):
    lats, lons, channels = kept.shape
    channels = 2 * channels
    state = jax.ShapeDtypeStruct((lats, lons, channels), jnp.bfloat16)
    spectrum = jax.ShapeDtypeStruct((lats, forward.shape[1], 2 * channels), jnp.bfloat16)
    return pl.pallas_call(
        pre_kernel,
        grid=(lats,),
        in_specs=[pl.BlockSpec(memory_space=pltpu.SMEM), by_row(kept.shape), by_row(kept.shape)]
        + [held(gain), held(forward)],
        out_specs=[by_row(state.shape), by_row(spectrum.shape)],
        out_shape=[state, spectrum],
        cost_estimate=pl.CostEstimate(
            flops=4 * state.size * forward.shape[1], bytes_accessed=4 * state.size, transcendentals=0
        ),
        name="pre",
    )(is_first.astype(jnp.int32).reshape(1), kept, arrived, gain, forward)


def call_post(returned, state, inverse, forward, params, gain_next):
    gain_one, gain_two, skip, first, second = params
    lats, lons, channels = state.shape
    weights = [inverse, forward, gain_one, gain_two]
    weights += [gain_one if gain_next is None else gain_next, skip, first, second]
    shapes = [jax.ShapeDtypeStruct(state.shape, jnp.bfloat16)]
    if gain_next is not None:
        shapes.append(jax.ShapeDtypeStruct(returned.shape, jnp.bfloat16))
    flops = 2 * state.size * (4 * forward.shape[1] + channels + 2 * first.shape[1])
    return pl.pallas_call(
        post_kernel,
        grid=(lats,),
        in_specs=[by_row(returned.shape), by_row(state.shape)] + [held(w) for w in weights],
        out_specs=[by_row(shape.shape) for shape in shapes],
        out_shape=shapes,
        cost_estimate=pl.CostEstimate(
            flops=4 * flops, bytes_accessed=8 * state.size, transcendentals=3 * state.size
        ),
        name="post",
    )(returned, state, *weights)


def swapped(value):
    return lax.ppermute(value, "section", [(0, 1), (1, 0)])


def split(centred, own_params, tables):
    is_first = lax.axis_index("section") == 0
    half = centred.shape[0] // 2
    forward, inverse, weighted, plain_table = tables
    forward_rows = jnp.transpose(forward, (1, 2, 0))
    inverse_rows = jnp.transpose(inverse, (0, 2, 1))

    def sides(value, other):
        return (jnp.where(is_first, value, other), jnp.where(is_first, other, value))

    gain_one, full_gain, skip_matrix, gain_two, first_matrix, second_matrix = own_params
    channels = skip_matrix.shape[0]
    hidden_units = first_matrix.shape[1]
    m_count = weighted.shape[1]
    own_gain = jnp.pad(jnp.stack([gain_one, gain_two]), ((0, 6), (0, 0)))
    gains = sides(own_gain, swapped(own_gain))
    pieces = []
    for index in range(half):
        low, high = (centred[index], centred[half + index])
        arrived = swapped(jnp.where(is_first, high, low))
        pieces.append((jnp.where(is_first, low, high), arrived))
    own_narrow = jnp.concatenate([skip_matrix, first_matrix, second_matrix], axis=1)
    own_filter = full_gain.reshape(-1, channels)
    narrow_there = swapped(own_narrow)
    filter_there = swapped(own_filter)

    def outward(spectrum):
        return lax.all_to_all(spectrum[None], "sht", split_axis=2, concat_axis=1, tiled=True)

    def middle(exchanged, filter_table):
        coeffs = jnp.einsum(
            "lmj,bjmq->blmq", weighted, exchanged, preferred_element_type=jnp.float32
        ).reshape(1, LMAX, m_count, 2, channels)
        filtered = apply_gain(coeffs, filter_table).astype(jnp.bfloat16)
        filtered = filtered.reshape(1, LMAX, m_count, 2 * channels)
        returned = jnp.einsum(
            "lmj,blmq->bjmq", plain_table, filtered, preferred_element_type=jnp.float32
        ).astype(jnp.bfloat16)
        return lax.all_to_all(returned, "sht", split_axis=1, concat_axis=2, tiled=True)[0]

    states, spectra = ([], [])
    for kept, arrived in pieces:
        state, spectrum = call_pre(is_first, kept, arrived, gains[0][0:1], forward_rows)
        states.append(state)
        spectra.append(spectrum)
    exchanged = [outward(spectrum) for spectrum in spectra]
    exchanged[0], filter_there = lax.optimization_barrier((exchanged[0], filter_there))
    exchanged[1], narrow_there = lax.optimization_barrier((exchanged[1], narrow_there))
    narrow = sides(own_narrow, narrow_there)
    filters = [f.reshape(full_gain.shape) for f in sides(own_filter, filter_there)]
    params = [
        (
            gains[b][0:1],
            gains[b][1:2],
            narrow[b][:, :channels],
            narrow[b][:, channels : channels + hidden_units],
            jnp.transpose(narrow[b][:, channels + hidden_units :]),
        )
        for b in range(2)
    ]
    returned = [middle(one, filters[0]) for one in exchanged]
    between = [
        call_post(one, state, inverse_rows, forward_rows, params[0], gains[1][0:1])
        for one, state in zip(returned, states)
    ]
    flats = [state.reshape(state.shape[0], -1) for state, _ in between]
    first_there = [lax.ppermute(flat, "section", [(1, 0)]) for flat in flats]
    exchanged = [outward(spectrum) for _, spectrum in between]
    exchanged[-1], first_there[0] = lax.optimization_barrier((exchanged[-1], first_there[0]))
    returned = [middle(one, filters[1]) for one in exchanged]
    for index in range(1, half):
        returned[index - 1], first_there[index] = lax.optimization_barrier(
            (returned[index - 1], first_there[index])
        )
    head, tail = ([], [])
    for index in range(half):
        there = first_there[index]
        (last,) = call_post(returned[index], between[index][0], inverse_rows, forward_rows, params[1], None)
        flat = last.reshape(last.shape[0], -1)
        head.append(jnp.where(is_first, flats[index], lax.ppermute(flat, "section", [(0, 1)])))
        tail.append(jnp.where(is_first, there, flat))
    return jnp.stack(head + tail)[None]


def per_device(
    analysis, perturbations, gain_first, spectral_gain, skip_weight, gain_second, mlp_in, mlp_out
):
    centred = recenter(analysis, perturbations)
    forward, inverse = fourier_tables(NLON, MMAX)
    m_count = MMAX // lax.axis_size("sht")
    legendre, weights = legendre_table(
        NLAT, LMAX, MMAX, NLON, lax.axis_index("sht") * m_count, m_count
    )
    weighted = (legendre * weights).astype(jnp.bfloat16)
    plain_table = legendre.astype(jnp.bfloat16)
    block = make_block(m_count, (forward, inverse, weighted, plain_table))
    own_params = (
        gain_first[0],
        spectral_gain[0].reshape(2, LMAX, C),
        skip_weight[0],
        gain_second[0],
        mlp_in[0],
        mlp_out[0],
    )
    if lax.axis_size("section") == 2 and centred.shape[0] % 2 == 0 and centred.shape[0] > 2:
        return split(centred, own_params, (forward, inverse, weighted, plain_table))
    return piped(centred, own_params, block)


def solution(mesh):
    return jax.shard_map(
        per_device,
        mesh=mesh,
        in_specs=(
            P("sht", None, "section"),
            P(None, "sht", None, "section"),
            P("section", None),
            P("section", None, None),
            P("section", None, None),
            P("section", None),
            P("section", None, None),
            P("section", None, None),
        ),
        out_specs=P("section", None, "sht", None),
        check_vma=False,
    )
```
